32 devices in a mesh: tp: 8 (over z, y), cp: 4 (over x, core).
Axes of the slice: x: 2, y: 2, z: 4, core: 2. Of those that a mesh axis runs over, the one named last changes fastest.
Arguments:
- tokens: int32 [4096], P('cp')
- pos: int32 [4096], P('cp')
- doc_id: int32 [4096], P('cp')
- dy: bfloat16 [4096, 2048], P('cp')
- table: bfloat16 [32256, 2048], P('tp')
- w_q: bfloat16 [2048, 2048], P(None, 'tp')
- w_k: bfloat16 [2048, 2048], P(None, 'tp')
- w_v: bfloat16 [2048, 2048], P(None, 'tp')
- w_o: bfloat16 [2048, 2048], P('tp')
- w_gate: bfloat16 [2048, 5504], P(None, 'tp')
- w_up: bfloat16 [2048, 5504], P(None, 'tp')
- w_down: bfloat16 [5504, 2048], P('tp')
- gain_one: bfloat16 [2048], replicated
- gain_two: bfloat16 [2048], replicated
- inv_freq: float32 [64], replicated
Outputs:
- output 1: bfloat16 [4096, 2048], P('cp')
- output 2: float32 [32256, 2048], P('tp')
- output 3: float32 [2048, 2048], P(None, 'tp')
- output 4: float32 [2048, 2048], P(None, 'tp')
- output 5: float32 [2048, 2048], P(None, 'tp')
- output 6: float32 [2048, 2048], P('tp')
- output 7: float32 [2048, 5504], P(None, 'tp')
- output 8: float32 [2048, 5504], P(None, 'tp')
- output 9: float32 [5504, 2048], P('tp')
- output 10: float32 [2048], replicated
- output 11: float32 [2048], replicated
All inputs are finite; a program needn't handle non-finite values.
Results may differ from the reference program's by a relative error of at most 0.0147249.
Values are sent between devices in bfloat16 or wider.
A program may use at most 1 GiB of HBM per device.

```python
import math
import jax
import jax.numpy as jnp
from jax import lax

VOCAB = 32256
MODEL_DIM = 2048
HEADS = 16
KV_HEADS = 16
HEAD_DIM = 128
FFN_DIM = 5504
TOK_BLOCK = 512
CP_SIZE = 4

TOKENS = 2 * CP_SIZE * TOK_BLOCK
GROUP = HEADS // KV_HEADS
HOT_COUNT = 2 ** 5
NORM_EPS = 1e-5
SCORE_SCALE = HEAD_DIM ** -0.5
NEG_BIG = -1e30


def slot_sequence():
    slot = jnp.arange(TOKENS)
    shard = slot // (2 * TOK_BLOCK)
    within = slot % (2 * TOK_BLOCK)
    block_no = jnp.where(within < TOK_BLOCK, shard, 2 * CP_SIZE - 1 - shard)
    return block_no * TOK_BLOCK + within % TOK_BLOCK


def draw_layout(key):
    keys = jax.random.split(key, 5)
    seq_pos = slot_sequence()
    cuts = jax.random.randint(keys[0], (CP_SIZE,), 1, TOKENS)
    after_cut = cuts[None, :] <= seq_pos[:, None]
    doc_id = jnp.sum(after_cut.astype(jnp.int32), axis=1)
    doc_start = jnp.max(jnp.where(after_cut, cuts[None, :], 0), axis=1)
    pos = (seq_pos - doc_start).astype(jnp.int32)
    hot_ids = jax.random.randint(keys[1], (HOT_COUNT,), 0, VOCAB // 8)
    hot_pick = jax.random.randint(keys[2], (TOKENS,), 0, HOT_COUNT)
    spread_ids = jax.random.randint(keys[3], (TOKENS,), 0, VOCAB)
    use_hot = jax.random.randint(keys[4], (TOKENS,), 0, 2)
    tokens = jnp.where(use_hot == 1, hot_ids[hot_pick], spread_ids)
    tokens = tokens.at[0].set(0).at[1].set(VOCAB - 1)
    return tokens, pos, doc_id.astype(jnp.int32)


def setup_inputs(seed: int = 0) -> dict:
    base = jax.random.key(seed)
    tokens, pos, doc_id = draw_layout(jax.random.fold_in(base, 1))
    keys = jax.random.split(jax.random.fold_in(base, 2), 14)

    def weight(which, fan_in, fan_out):
        return (jax.random.normal(keys[which], (fan_in, fan_out), jnp.float32) * fan_in ** -0.5).astype(jnp.bfloat16)

    def gain(which):
        return (1.0 + 0.25 * jax.random.normal(keys[which], (MODEL_DIM,), jnp.float32)).astype(jnp.bfloat16)

    log_theta = jax.random.uniform(keys[11], (), jnp.float32, math.log(1e4), math.log(5e5))
    exponent = jnp.arange(HEAD_DIM // 2, dtype=jnp.float32) * (2.0 / HEAD_DIM)
    jitter = jax.random.uniform(keys[12], (HEAD_DIM // 2,), jnp.float32, 0.9, 1.1)
    return {
        "tokens": tokens,
        "pos": pos,
        "doc_id": doc_id,
        "dy": jax.random.normal(keys[0], (TOKENS, MODEL_DIM), jnp.float32).astype(jnp.bfloat16),
        "table": jax.random.normal(keys[1], (VOCAB, MODEL_DIM), jnp.float32).astype(jnp.bfloat16),
        "w_q": weight(2, MODEL_DIM, HEADS * HEAD_DIM),
        "w_k": weight(3, MODEL_DIM, KV_HEADS * HEAD_DIM),
        "w_v": weight(4, MODEL_DIM, KV_HEADS * HEAD_DIM),
        "w_o": weight(5, HEADS * HEAD_DIM, MODEL_DIM),
        "w_gate": weight(6, MODEL_DIM, FFN_DIM),
        "w_up": weight(7, MODEL_DIM, FFN_DIM),
        "w_down": weight(8, FFN_DIM, MODEL_DIM),
        "gain_one": gain(9),
        "gain_two": gain(10),
        "inv_freq": jnp.exp(-log_theta * exponent) * jitter,
    }


def to_bf16(feats):
    return feats.astype(jnp.bfloat16).astype(jnp.float32)


def rms_norm(feats, gain_vec):
    return feats * lax.rsqrt(jnp.mean(feats * feats, axis=-1, keepdims=True) + NORM_EPS) * gain_vec


def rotate(tensor_in, cosine, sine):
    half = tensor_in.shape[-1] // 2
    first = tensor_in[..., :half]
    second = tensor_in[..., half:]
    return jnp.concatenate([first * cosine - second * sine, second * cosine + first * sine], axis=-1)


def forward_pass(params, tokens, pos, doc_id, inv_freq):
    table, w_q, w_k, w_v, w_o, w_gate, w_up, w_down, gain_one, gain_two = params
    embed = jnp.take(table, tokens, axis=0)
    act_one = to_bf16(rms_norm(embed, gain_one))
    angle = pos.astype(jnp.float32)[:, None, None] * inv_freq
    cosine = jnp.cos(angle)
    sine = jnp.sin(angle)
    query = jnp.dot(act_one, w_q, preferred_element_type=jnp.float32).reshape(TOKENS, HEADS, HEAD_DIM)
    query = to_bf16(rotate(query, cosine, sine)).reshape(2 * CP_SIZE, TOK_BLOCK, KV_HEADS, GROUP, HEAD_DIM)
    key_all = jnp.dot(act_one, w_k, preferred_element_type=jnp.float32).reshape(TOKENS, KV_HEADS, HEAD_DIM)
    key_all = to_bf16(rotate(key_all, cosine, sine))
    value_all = to_bf16(jnp.dot(act_one, w_v, preferred_element_type=jnp.float32)).reshape(TOKENS, KV_HEADS, HEAD_DIM)
    seq_pos = slot_sequence()

    def attend(block):
        query_blk, seq_blk, doc_blk = block
        scores = jnp.einsum("qkgd,skd->kgqs", query_blk, key_all) * SCORE_SCALE
        allowed = (doc_blk[:, None] == doc_id[None, :]) & (seq_pos[None, :] <= seq_blk[:, None])
        attn_prob = jax.nn.softmax(jnp.where(allowed, scores, NEG_BIG), axis=-1)
        return jnp.einsum("kgqs,skd->qkgd", to_bf16(attn_prob), value_all)

    blocks = (query, seq_pos.reshape(2 * CP_SIZE, TOK_BLOCK), doc_id.reshape(2 * CP_SIZE, TOK_BLOCK))
    attended = to_bf16(lax.map(jax.checkpoint(attend), blocks)).reshape(TOKENS, HEADS * HEAD_DIM)
    residual = embed + jnp.dot(attended, w_o, preferred_element_type=jnp.float32)
    act_two = to_bf16(rms_norm(residual, gain_two))
    gate = jnp.dot(act_two, w_gate, preferred_element_type=jnp.float32)
    hidden = to_bf16(jax.nn.silu(gate) * jnp.dot(act_two, w_up, preferred_element_type=jnp.float32))
    return residual + jnp.dot(hidden, w_down, preferred_element_type=jnp.float32)


def reference(tokens, pos, doc_id, dy, table, w_q, w_k, w_v, w_o, w_gate, w_up, w_down, gain_one, gain_two, inv_freq):
    params = tuple(weight.astype(jnp.float32) for weight in (table, w_q, w_k, w_v, w_o, w_gate, w_up, w_down, gain_one, gain_two))
    layer_out, pullback = jax.vjp(lambda *weights: forward_pass(weights, tokens, pos, doc_id, inv_freq), *params)
    grads = pullback(dy.astype(jnp.float32))
    return (layer_out.astype(jnp.bfloat16), grads[0], grads[1], grads[2], grads[3], grads[4], grads[5], grads[6], grads[7], grads[8], grads[9])
```

```python
import functools

import jax
import jax.numpy as jnp
from jax import lax
from jax.experimental import pallas as pl
from jax.experimental.pallas import tpu as pltpu
from jax.sharding import PartitionSpec as P

NORM_EPS = 1e-5
NEG_BIG = -1e30


def rms_stats(feats):
    inv_rms = lax.rsqrt(jnp.mean(feats * feats, axis=-1, keepdims=True) + NORM_EPS)
    return feats * inv_rms, inv_rms


def rms_back(d_normed, normed, inv_rms):
    return inv_rms * (d_normed - normed * jnp.mean(d_normed * normed, axis=-1, keepdims=True))


def rotate(tensor_in, cosine, sine):
    half = tensor_in.shape[-1] // 2
    first = tensor_in[..., :half]
    second = tensor_in[..., half:]
    return jnp.concatenate([first * cosine - second * sine, second * cosine + first * sine], axis=-1)


def to_bf16(feats):
    return feats.astype(jnp.bfloat16).astype(jnp.float32)


def slot_sequence(slot, block_len, cp_count):
    shard = slot // (2 * block_len)
    within = slot % (2 * block_len)
    block_no = jnp.where(within < block_len, shard, 2 * cp_count - 1 - shard)
    return block_no * block_len + within % block_len


KEY_STEP = 512
QUERY_STEP = 256
NT = (((1,), (1,)), ((), ()))
NN = (((1,), (0,)), ((), ()))


def block_number(index, cp_count):
    shard = index // 2
    return jnp.where(index % 2 == 0, shard, 2 * cp_count - 1 - shard)


def block_scores(key_ref, query, low, high, index, cp_count, scale):
    first = block_number(index, cp_count) * KEY_STEP
    keys = key_ref[pl.ds(pl.multiple_of(index * KEY_STEP, KEY_STEP), KEY_STEP), :]
    scores = lax.dot_general(keys, query, NT, preferred_element_type=jnp.float32) * scale
    seq = first + lax.broadcasted_iota(jnp.int32, scores.shape, 0)
    return jnp.where((seq >= low) & (seq <= high), scores, NEG_BIG)


def block_needed(index, tile_low, tile_high, cp_count):
    first = block_number(index, cp_count) * KEY_STEP
    return (first <= tile_high) & (first + KEY_STEP > tile_low)


def attend_kernel(cp_count, scale, bounds, query_ref, key_ref, value_t_ref, low_ref, high_ref, out_ref, top_ref, norm_ref, scores_ref):
    tile = pl.program_id(1)
    tile_low = bounds[0, tile]
    tile_high = bounds[1, tile]
    query = query_ref[...]
    low = low_ref[...]
    high = high_ref[...]
    count = key_ref.shape[0] // KEY_STEP
    step = query.shape[0]
    top_ref[0] = jnp.full((1, step), NEG_BIG, jnp.float32)

    def rows_of(index):
        return pl.ds(pl.multiple_of(index * KEY_STEP, KEY_STEP), KEY_STEP)

    @pl.loop(0, count)
    def _(index):
        @pl.when(block_needed(index, tile_low, tile_high, cp_count))
        def _():
            scores = block_scores(key_ref, query, low, high, index, cp_count, scale)
            scores_ref[rows_of(index), :] = scores
            top_ref[0] = jnp.maximum(top_ref[0], jnp.max(scores, axis=0, keepdims=True))

    norm_ref[0] = jnp.zeros((1, step), jnp.float32)

    @pl.loop(0, count)
    def _(index):
        @pl.when(block_needed(index, tile_low, tile_high, cp_count))
        def _():
            weight = jnp.exp(scores_ref[rows_of(index), :] - top_ref[0])
            scores_ref[rows_of(index), :] = weight
            norm_ref[0] = norm_ref[0] + jnp.sum(weight, axis=0, keepdims=True)

    norm_ref[0] = 1.0 / norm_ref[0]
    out_ref[...] = jnp.zeros_like(out_ref)

    @pl.loop(0, count)
    def _(index):
        @pl.when(block_needed(index, tile_low, tile_high, cp_count))
        def _():
            prob = (scores_ref[rows_of(index), :] * norm_ref[0]).astype(jnp.bfloat16)
            out_ref[...] += lax.dot_general(value_t_ref[:, rows_of(index)], prob, NN, preferred_element_type=jnp.float32)


def attend_back_kernel(cp_count, scale, bounds, query_ref, key_ref, key_t_ref, value_ref, d_out_ref, low_ref, high_ref, top_ref, norm_ref, d_query_ref, d_kv_ref, prob_ref, d_prob_ref, dot_ref):
    tile = pl.program_id(1)
    tile_low = bounds[0, tile]
    tile_high = bounds[1, tile]
    query = query_ref[...]
    d_out = d_out_ref[...]
    low = low_ref[...]
    high = high_ref[...]
    count = key_ref.shape[0] // KEY_STEP
    step = query.shape[0]

    def rows_of(index):
        return pl.ds(pl.multiple_of(index * KEY_STEP, KEY_STEP), KEY_STEP)

    @pl.when(tile == 0)
    def _():
        d_kv_ref[...] = jnp.zeros_like(d_kv_ref)

    dot_ref[...] = jnp.zeros((1, step), jnp.float32)

    @pl.loop(0, count)
    def _(index):
        @pl.when(block_needed(index, tile_low, tile_high, cp_count))
        def _():
            scores = block_scores(key_ref, query, low, high, index, cp_count, scale)
            prob = jnp.exp(scores - top_ref[0]) * norm_ref[0]
            d_prob = lax.dot_general(value_ref[rows_of(index), :], d_out, NT, preferred_element_type=jnp.float32)
            d_prob = d_prob.astype(jnp.bfloat16).astype(jnp.float32)
            prob_ref[rows_of(index), :] = prob
            d_prob_ref[rows_of(index), :] = d_prob
            dot_ref[...] += jnp.sum(prob * d_prob, axis=0, keepdims=True)

    d_query_ref[...] = jnp.zeros_like(d_query_ref)

    @pl.loop(0, count)
    def _(index):
        @pl.when(block_needed(index, tile_low, tile_high, cp_count))
        def _():
            prob = prob_ref[rows_of(index), :]
            d_scores = prob * (d_prob_ref[rows_of(index), :] - dot_ref[...]) * scale
            d_scores = d_scores.astype(jnp.bfloat16)
            d_query_ref[...] += lax.dot_general(key_t_ref[:, rows_of(index)], d_scores, NN, preferred_element_type=jnp.float32)
            d_kv_ref[0, rows_of(index), :] += lax.dot_general(d_scores, query, NN, preferred_element_type=jnp.float32)
            d_kv_ref[1, rows_of(index), :] += lax.dot_general(prob.astype(jnp.bfloat16), d_out, NN, preferred_element_type=jnp.float32)


def attend(cp_count, scale, bounds, query, key_value, value_t, low, high):
    span, local_dim = query.shape
    total = key_value.shape[0]
    head_dim = 128
    heads = local_dim // head_dim
    step = QUERY_STEP
    tiles = span // step
    row = pl.BlockSpec((1, step), lambda h, i, b: (0, i))
    stat = pl.BlockSpec((1, 1, step), lambda h, i, b: (h, 0, i))
    out_t, top, norm = pl.pallas_call(
        functools.partial(attend_kernel, cp_count, scale),
        grid_spec=pltpu.PrefetchScalarGridSpec(
            num_scalar_prefetch=1,
            grid=(heads, tiles),
            in_specs=[
                pl.BlockSpec((step, head_dim), lambda h, i, b: (i, h)),
                pl.BlockSpec((total, head_dim), lambda h, i, b: (0, h)),
                pl.BlockSpec((head_dim, total), lambda h, i, b: (heads + h, 0)),
                row,
                row,
            ],
            out_specs=[pl.BlockSpec((head_dim, step), lambda h, i, b: (h, i)), stat, stat],
            scratch_shapes=[pltpu.VMEM((total, step), jnp.float32)],
        ),
        out_shape=[
            jax.ShapeDtypeStruct((local_dim, span), jnp.float32),
            jax.ShapeDtypeStruct((heads, 1, span), jnp.float32),
            jax.ShapeDtypeStruct((heads, 1, span), jnp.float32),
        ],
        compiler_params=pltpu.CompilerParams(vmem_limit_bytes=40 * 2**20),
        cost_estimate=pl.CostEstimate(flops=6 * span * total * local_dim, bytes_accessed=8 * total * local_dim, transcendentals=span * total * heads),
        name="attend",
    )(bounds, query, key_value, value_t, low, high)
    return out_t, top, norm


def attend_back(cp_count, scale, bounds, query, key_value, key_t, d_out, low, high, top, norm):
    span, local_dim = query.shape
    total = key_value.shape[0]
    head_dim = 128
    heads = local_dim // head_dim
    step = QUERY_STEP
    tiles = span // step
    row = pl.BlockSpec((1, step), lambda h, i, b: (0, i))
    stat = pl.BlockSpec((1, 1, step), lambda h, i, b: (h, 0, i))
    tall = pl.BlockSpec((step, head_dim), lambda h, i, b: (i, h))
    return pl.pallas_call(
        functools.partial(attend_back_kernel, cp_count, scale),
        grid_spec=pltpu.PrefetchScalarGridSpec(
            num_scalar_prefetch=1,
            grid=(heads, tiles),
            in_specs=[
                tall,
                pl.BlockSpec((total, head_dim), lambda h, i, b: (0, h)),
                pl.BlockSpec((head_dim, total), lambda h, i, b: (h, 0)),
                pl.BlockSpec((total, head_dim), lambda h, i, b: (0, heads + h)),
                tall,
                row,
                row,
                stat,
                stat,
            ],
            out_specs=[pl.BlockSpec((head_dim, step), lambda h, i, b: (h, i)), pl.BlockSpec((2, total, head_dim), lambda h, i, b: (0, 0, h))],
            scratch_shapes=[pltpu.VMEM((total, step), jnp.float32), pltpu.VMEM((total, step), jnp.float32), pltpu.VMEM((1, step), jnp.float32)],
        ),
        out_shape=[
            jax.ShapeDtypeStruct((local_dim, span), jnp.float32),
            jax.ShapeDtypeStruct((2, total, local_dim), jnp.float32),
        ],
        compiler_params=pltpu.CompilerParams(vmem_limit_bytes=48 * 2**20),
        cost_estimate=pl.CostEstimate(flops=14 * span * total * local_dim, bytes_accessed=16 * total * local_dim, transcendentals=span * total * heads),
        name="attend_back",
    )(bounds, query, key_value, key_t, key_value, d_out, low, high, top, norm)


def solution(mesh):
    cp_count = mesh.shape["cp"]
    tp_count = mesh.shape["tp"]
    core_swap = [(i, i ^ 1) for i in range(cp_count)]
    chip_swap = [(i, i ^ (cp_count // 2)) for i in range(cp_count)]

    def device_step(tokens, pos, doc_id, dy, table, w_q, w_k, w_v, w_o, w_gate, w_up, w_down, gain_one, gain_two, inv_freq):
        span = tokens.shape[0]
        part = span // tp_count
        total = span * cp_count
        rows = table.shape[0]
        width = table.shape[1]
        head_dim = 2 * inv_freq.shape[0]
        heads = w_q.shape[1] // head_dim
        local_dim = heads * head_dim
        scale = head_dim ** -0.5
        tp_rank = lax.axis_index("tp")
        cp_rank = lax.axis_index("cp")
        core = cp_rank % 2
        gain_a = gain_one.astype(jnp.float32)
        gain_b = gain_two.astype(jnp.float32)

        def cp_sum(partial):
            half = partial.shape[0] // 2
            mine = lax.dynamic_slice_in_dim(partial, core * half, half, 0)
            other = lax.dynamic_slice_in_dim(partial, (1 - core) * half, half, 0)
            chip_half = mine + lax.ppermute(other, "cp", core_swap)
            total_half = chip_half + lax.ppermute(chip_half, "cp", chip_swap)
            other_half = lax.ppermute(total_half, "cp", core_swap)
            low = jnp.where(core == 0, total_half, other_half)
            high = jnp.where(core == 0, other_half, total_half)
            return jnp.concatenate([low, high], axis=0)

        ring_order = (tp_rank - jnp.arange(tp_count)) % tp_count
        half_dim = local_dim // 2
        wo_half = lax.dynamic_slice_in_dim(w_o, core * half_dim, half_dim, 0)
        wo_parts = [wo_half]
        for shift in range(1, tp_count):
            wo_parts.append(lax.ppermute(wo_half, "tp", [(i, (i + shift) % tp_count) for i in range(tp_count)]))
        wo_mine = jnp.concatenate(wo_parts, axis=0)
        wo_other = lax.ppermute(wo_mine, "cp", core_swap)
        wo_ring = jnp.concatenate([wo_mine, wo_other], axis=0)

        def to_ring(blocks):
            picked_blocks = jnp.take(blocks, ring_order, axis=0).reshape(tp_count, part, 2, half_dim)
            both = jnp.where(core == 0, picked_blocks, picked_blocks[:, :, ::-1])
            return both.transpose(1, 2, 0, 3).reshape(part, tp_count * local_dim)

        def from_ring(flat):
            both = flat.reshape(part, 2, tp_count, half_dim).transpose(2, 0, 1, 3)
            both = jnp.where(core == 0, both, both[:, :, ::-1]).reshape(tp_count, part, local_dim)
            return jnp.take(both, ring_order, axis=0)

        local_ids = tokens - tp_rank * rows
        owned = (local_ids >= 0) & (local_ids < rows)
        safe_ids = jnp.where(owned, local_ids, 0)
        picked = jnp.where(owned[:, None], jnp.take(table, safe_ids, axis=0), jnp.zeros((), jnp.bfloat16))
        embed = lax.psum_scatter(picked, "tp", scatter_dimension=0, tiled=True).astype(jnp.float32)

        normed_a, inv_a = rms_stats(embed)
        act_a = lax.all_gather((normed_a * gain_a).astype(jnp.bfloat16), "tp", axis=0, tiled=True)
        angle = pos.astype(jnp.float32)[:, None, None] * inv_freq
        cosine = jnp.cos(angle)
        sine = jnp.sin(angle)
        query = jnp.dot(act_a, w_q, preferred_element_type=jnp.float32).reshape(span, heads, head_dim)
        query = rotate(query, cosine, sine).astype(jnp.bfloat16).reshape(span, local_dim)
        key_loc = jnp.dot(act_a, w_k, preferred_element_type=jnp.float32).reshape(span, heads, head_dim)
        key_loc = rotate(key_loc, cosine, sine).astype(jnp.bfloat16)
        value_loc = jnp.dot(act_a, w_v, preferred_element_type=jnp.float32).astype(jnp.bfloat16)
        key_value = jnp.concatenate([key_loc.reshape(span, local_dim), value_loc], axis=1)
        kv_all = lax.all_gather(key_value, "cp", axis=0, tiled=True)
        kv_all_t = kv_all.T
        token_all = lax.all_gather(tokens, "cp", axis=0, tiled=True)
        q_seq = slot_sequence(cp_rank * span + jnp.arange(span, dtype=jnp.int32), span // 2, cp_count)
        q_first = q_seq - pos
        bounds = jnp.stack([jnp.min(q_first.reshape(-1, QUERY_STEP), axis=1), jnp.max(q_seq.reshape(-1, QUERY_STEP), axis=1)])
        low = q_first.reshape(1, span)
        high = q_seq.reshape(1, span)
        out_t, top, norm = attend(cp_count, scale, bounds, query, kv_all, kv_all_t, low, high)
        attended = out_t.T.astype(jnp.bfloat16)
        att_rows = lax.all_to_all(attended.reshape(tp_count, part, local_dim), "tp", 0, 0)
        residual = embed + jnp.dot(to_ring(att_rows), wo_ring, preferred_element_type=jnp.float32)
        normed_b, inv_b = rms_stats(residual)
        act_b = lax.all_gather((normed_b * gain_b).astype(jnp.bfloat16), "tp", axis=0, tiled=True)
        gate = jnp.dot(act_b, w_gate, preferred_element_type=jnp.float32)
        up_val = jnp.dot(act_b, w_up, preferred_element_type=jnp.float32)
        gate_sig = jax.nn.sigmoid(gate)
        hidden = (gate * gate_sig * up_val).astype(jnp.bfloat16)

        d_hidden = to_bf16(jnp.einsum("td,fd->tf", dy, w_down, preferred_element_type=jnp.float32))
        d_gate = (d_hidden * up_val * gate_sig * (1.0 + gate * (1.0 - gate_sig))).astype(jnp.bfloat16)
        d_up = (d_hidden * gate * gate_sig).astype(jnp.bfloat16)
        d_act_b = jnp.einsum("tf,df->td", d_gate, w_gate, preferred_element_type=jnp.float32)
        d_act_b = d_act_b + jnp.einsum("tf,df->td", d_up, w_up, preferred_element_type=jnp.float32)
        d_act_b = to_bf16(lax.psum_scatter(d_act_b, "tp", scatter_dimension=0, tiled=True))
        grad_gain_b = jnp.sum(d_act_b * normed_b, axis=0)
        dy_part = lax.dynamic_slice_in_dim(dy, tp_rank * part, part, 0).astype(jnp.float32)
        d_resid = dy_part + rms_back(d_act_b * gain_b, normed_b, inv_b)
        d_resid_b = d_resid.astype(jnp.bfloat16)
        d_att_rows = jnp.einsum("td,cd->tc", d_resid_b, wo_ring, preferred_element_type=jnp.float32)
        d_att = lax.all_to_all(from_ring(d_att_rows.astype(jnp.bfloat16)), "tp", 0, 0)
        d_att = d_att.reshape(span, local_dim)

        hidden_late, d_att = lax.optimization_barrier((hidden, d_att))
        grad_down = cp_sum(jnp.einsum("tf,td->fd", hidden, dy, preferred_element_type=jnp.float32))
        grad_gate = cp_sum(jnp.einsum("td,tf->df", act_b, d_gate, preferred_element_type=jnp.float32))
        grad_up = cp_sum(jnp.einsum("td,tf->df", act_b, d_up, preferred_element_type=jnp.float32))
        layer_part = jnp.dot(hidden_late, w_down, preferred_element_type=jnp.float32)
        layer_part = residual + lax.psum_scatter(layer_part, "tp", scatter_dimension=0, tiled=True)
        layer_out = lax.all_gather(layer_part.astype(jnp.bfloat16), "tp", axis=0, tiled=True)
        resid_all = lax.all_gather(d_resid_b, "tp", axis=0, tiled=True)
        grad_out = cp_sum(jnp.einsum("tc,td->cd", attended, resid_all, preferred_element_type=jnp.float32))

        d_query_t, d_kv_all = attend_back(cp_count, scale, bounds, query, kv_all, kv_all_t, d_att, low, high, top, norm)
        d_query = d_query_t.T.reshape(span, heads, head_dim)
        d_kv_all = d_kv_all.reshape(2, cp_count // 2, 2, span, local_dim)
        chip = cp_rank // 2
        mate_kv = lax.dynamic_index_in_dim(d_kv_all, 1 - core, 2, keepdims=False)
        own_kv = lax.dynamic_index_in_dim(d_kv_all, core, 2, keepdims=False)
        chip_kv = own_kv + lax.ppermute(mate_kv, "cp", core_swap)
        far_kv = lax.dynamic_index_in_dim(chip_kv, 1 - chip, 1, keepdims=False)
        d_kv = lax.dynamic_index_in_dim(chip_kv, chip, 1, keepdims=False) + lax.ppermute(far_kv, "cp", chip_swap)
        d_key = d_kv[0].reshape(span, heads, head_dim)
        d_value = d_kv[1]
        d_q_pre = rotate(to_bf16(d_query), cosine, -sine)
        d_q_pre = d_q_pre.astype(jnp.bfloat16).reshape(span, local_dim)
        d_k_pre = rotate(to_bf16(d_key), cosine, -sine).astype(jnp.bfloat16).reshape(span, local_dim)
        d_v_pre = d_value.astype(jnp.bfloat16).reshape(span, local_dim)
        grad_q = cp_sum(jnp.einsum("td,tc->dc", act_a, d_q_pre, preferred_element_type=jnp.float32))
        grad_k = cp_sum(jnp.einsum("td,tc->dc", act_a, d_k_pre, preferred_element_type=jnp.float32))
        grad_v = cp_sum(jnp.einsum("td,tc->dc", act_a, d_v_pre, preferred_element_type=jnp.float32))
        d_act_a = jnp.einsum("tc,dc->td", d_q_pre, w_q, preferred_element_type=jnp.float32)
        d_act_a = d_act_a + jnp.einsum("tc,dc->td", d_k_pre, w_k, preferred_element_type=jnp.float32)
        d_act_a = d_act_a + jnp.einsum("tc,dc->td", d_v_pre, w_v, preferred_element_type=jnp.float32)
        d_act_a = to_bf16(lax.psum_scatter(d_act_a, "tp", scatter_dimension=0, tiled=True))
        grad_gain_a = jnp.sum(d_act_a * normed_a, axis=0)
        d_embed = d_resid + rms_back(d_act_a * gain_a, normed_a, inv_a)
        embed_all = lax.all_gather(d_embed, ("cp", "tp"), axis=0, tiled=True)
        all_ids = token_all - tp_rank * rows
        drop_ids = jnp.where((all_ids >= 0) & (all_ids < rows), all_ids, rows)
        grad_table = jnp.zeros((rows, width), jnp.float32).at[drop_ids].add(embed_all, mode="drop")
        gains = lax.psum(jnp.stack([grad_gain_a, grad_gain_b]), ("tp", "cp"))
        return (layer_out, grad_table, grad_q, grad_k, grad_v, grad_out, grad_gate, grad_up, grad_down, gains[0], gains[1])

    col_spec = P(None, "tp")
    row_spec = P("tp", None)
    tok_spec = P("cp")
    rep_spec = P(None)
    in_specs = (tok_spec, tok_spec, tok_spec, P("cp", None), row_spec, col_spec, col_spec, col_spec, row_spec, col_spec, col_spec, row_spec, rep_spec, rep_spec, rep_spec)
    out_specs = (P("cp", None), row_spec, col_spec, col_spec, col_spec, row_spec, col_spec, col_spec, row_spec, rep_spec, rep_spec)
    return jax.shard_map(device_step, mesh=mesh, in_specs=in_specs, out_specs=out_specs, check_vma=False)
```

```python
import functools

import jax
import jax.numpy as jnp
from jax import lax
from jax.experimental import pallas as pl
from jax.experimental.pallas import tpu as pltpu
from jax.sharding import PartitionSpec as P


NORM_EPS = 1e-5
NEG_BIG = -1e30


def rms_stats(feats):
    inv_rms = lax.rsqrt(jnp.mean(feats * feats, axis=-1, keepdims=True) + NORM_EPS)
    return feats * inv_rms, inv_rms


def rms_back(d_normed, normed, inv_rms):
    return inv_rms * (d_normed - normed * jnp.mean(d_normed * normed, axis=-1, keepdims=True))


def rotate(tensor_in, cosine, sine):
    half = tensor_in.shape[-1] // 2
    first = tensor_in[..., :half]
    second = tensor_in[..., half:]
    return jnp.concatenate([first * cosine - second * sine, second * cosine + first * sine], axis=-1)


def to_bf16(feats):
    return feats.astype(jnp.bfloat16).astype(jnp.float32)


def slot_sequence(slot, block_len, cp_count):
    shard = slot // (2 * block_len)
    within = slot % (2 * block_len)
    block_no = jnp.where(within < block_len, shard, 2 * cp_count - 1 - shard)
    return block_no * block_len + within % block_len


KEY_STEP = 512
QUERY_STEP = 256
NT = (((1,), (1,)), ((), ()))
NN = (((1,), (0,)), ((), ()))


def block_number(index, cp_count):
    shard = index // 2
    return jnp.where(index % 2 == 0, shard, 2 * cp_count - 1 - shard)


def block_scores(key_ref, query, low, high, index, cp_count, scale):
    first = block_number(index, cp_count) * KEY_STEP
    keys = key_ref[pl.ds(pl.multiple_of(index * KEY_STEP, KEY_STEP), KEY_STEP), :]
    scores = lax.dot_general(keys, query, NT, preferred_element_type=jnp.float32) * scale
    seq = first + lax.broadcasted_iota(jnp.int32, scores.shape, 0)
    return jnp.where((seq >= low) & (seq <= high), scores, NEG_BIG)


def block_needed(index, tile_low, tile_high, cp_count):
    first = block_number(index, cp_count) * KEY_STEP
    return (first <= tile_high) & (first + KEY_STEP > tile_low)


def attend_kernel(cp_count, scale, bounds, query_ref, key_ref, value_t_ref, low_ref, high_ref, out_ref, top_ref, norm_ref, scores_ref):
    tile = pl.program_id(1)
    tile_low = bounds[0, tile]
    tile_high = bounds[1, tile]
    query = query_ref[...]
    low = low_ref[...]
    high = high_ref[...]
    count = key_ref.shape[0] // KEY_STEP
    step = query.shape[0]
    top_ref[0] = jnp.full((1, step), NEG_BIG, jnp.float32)

    def rows_of(index):
        return pl.ds(pl.multiple_of(index * KEY_STEP, KEY_STEP), KEY_STEP)

    @pl.loop(0, count)
    def _(index):
        @pl.when(block_needed(index, tile_low, tile_high, cp_count))
        def _():
            scores = block_scores(key_ref, query, low, high, index, cp_count, scale)
            scores_ref[rows_of(index), :] = scores
            top_ref[0] = jnp.maximum(top_ref[0], jnp.max(scores, axis=0, keepdims=True))

    norm_ref[0] = jnp.zeros((1, step), jnp.float32)

    @pl.loop(0, count)
    def _(index):
        @pl.when(block_needed(index, tile_low, tile_high, cp_count))
        def _():
            weight = jnp.exp(scores_ref[rows_of(index), :] - top_ref[0])
            scores_ref[rows_of(index), :] = weight
            norm_ref[0] = norm_ref[0] + jnp.sum(weight, axis=0, keepdims=True)

    norm_ref[0] = 1.0 / norm_ref[0]
    out_ref[...] = jnp.zeros_like(out_ref)

    @pl.loop(0, count)
    def _(index):
        @pl.when(block_needed(index, tile_low, tile_high, cp_count))
        def _():
            prob = (scores_ref[rows_of(index), :] * norm_ref[0]).astype(jnp.bfloat16)
            out_ref[...] += lax.dot_general(value_t_ref[:, rows_of(index)], prob, NN, preferred_element_type=jnp.float32)


def attend_back_kernel(cp_count, scale, bounds, query_ref, key_ref, key_t_ref, value_ref, d_out_ref, low_ref, high_ref, top_ref, norm_ref, d_query_ref, d_kv_ref, prob_ref, d_prob_ref, dot_ref):
    tile = pl.program_id(1)
    tile_low = bounds[0, tile]
    tile_high = bounds[1, tile]
    query = query_ref[...]
    d_out = d_out_ref[...]
    low = low_ref[...]
    high = high_ref[...]
    count = key_ref.shape[0] // KEY_STEP
    step = query.shape[0]

    def rows_of(index):
        return pl.ds(pl.multiple_of(index * KEY_STEP, KEY_STEP), KEY_STEP)

    @pl.when(tile == 0)
    def _():
        d_kv_ref[...] = jnp.zeros_like(d_kv_ref)

    dot_ref[...] = jnp.zeros((1, step), jnp.float32)

    @pl.loop(0, count)
    def _(index):
        @pl.when(block_needed(index, tile_low, tile_high, cp_count))
        def _():
            scores = block_scores(key_ref, query, low, high, index, cp_count, scale)
            prob = jnp.exp(scores - top_ref[0]) * norm_ref[0]
            d_prob = lax.dot_general(value_ref[rows_of(index), :], d_out, NT, preferred_element_type=jnp.float32)
            d_prob = d_prob.astype(jnp.bfloat16).astype(jnp.float32)
            prob_ref[rows_of(index), :] = prob
            d_prob_ref[rows_of(index), :] = d_prob
            dot_ref[...] += jnp.sum(prob * d_prob, axis=0, keepdims=True)

    d_query_ref[...] = jnp.zeros_like(d_query_ref)

    @pl.loop(0, count)
    def _(index):
        @pl.when(block_needed(index, tile_low, tile_high, cp_count))
        def _():
            prob = prob_ref[rows_of(index), :]
            d_scores = prob * (d_prob_ref[rows_of(index), :] - dot_ref[...]) * scale
            d_scores = d_scores.astype(jnp.bfloat16)
            d_query_ref[...] += lax.dot_general(key_t_ref[:, rows_of(index)], d_scores, NN, preferred_element_type=jnp.float32)
            d_kv_ref[0, rows_of(index), :] += lax.dot_general(d_scores, query, NN, preferred_element_type=jnp.float32)
            d_kv_ref[1, rows_of(index), :] += lax.dot_general(prob.astype(jnp.bfloat16), d_out, NN, preferred_element_type=jnp.float32)


def attend(cp_count, scale, bounds, query, key_value, value_t, low, high):
    span, local_dim = query.shape
    total = key_value.shape[0]
    head_dim = 128
    heads = local_dim // head_dim
    step = QUERY_STEP
    tiles = span // step
    row = pl.BlockSpec((1, step), lambda h, i, b: (0, i))
    stat = pl.BlockSpec((1, 1, step), lambda h, i, b: (h, 0, i))
    out_t, top, norm = pl.pallas_call(
        functools.partial(attend_kernel, cp_count, scale),
        grid_spec=pltpu.PrefetchScalarGridSpec(
            num_scalar_prefetch=1,
            grid=(heads, tiles),
            in_specs=[
                pl.BlockSpec((step, head_dim), lambda h, i, b: (i, h)),
                pl.BlockSpec((total, head_dim), lambda h, i, b: (0, h)),
                pl.BlockSpec((head_dim, total), lambda h, i, b: (heads + h, 0)),
                row,
                row,
            ],
            out_specs=[pl.BlockSpec((head_dim, step), lambda h, i, b: (h, i)), stat, stat],
            scratch_shapes=[pltpu.VMEM((total, step), jnp.float32)],
        ),
        out_shape=[
            jax.ShapeDtypeStruct((local_dim, span), jnp.float32),
            jax.ShapeDtypeStruct((heads, 1, span), jnp.float32),
            jax.ShapeDtypeStruct((heads, 1, span), jnp.float32),
        ],
        compiler_params=pltpu.CompilerParams(vmem_limit_bytes=40 * 2**20),
        cost_estimate=pl.CostEstimate(flops=6 * span * total * local_dim, bytes_accessed=8 * total * local_dim, transcendentals=span * total * heads),
        name="attend",
    )(bounds, query, key_value, value_t, low, high)
    return out_t, top, norm


def attend_back(cp_count, scale, bounds, query, key_value, key_t, d_out, low, high, top, norm):
    span, local_dim = query.shape
    total = key_value.shape[0]
    head_dim = 128
    heads = local_dim // head_dim
    step = QUERY_STEP
    tiles = span // step
    row = pl.BlockSpec((1, step), lambda h, i, b: (0, i))
    stat = pl.BlockSpec((1, 1, step), lambda h, i, b: (h, 0, i))
    tall = pl.BlockSpec((step, head_dim), lambda h, i, b: (i, h))
    return pl.pallas_call(
        functools.partial(attend_back_kernel, cp_count, scale),
        grid_spec=pltpu.PrefetchScalarGridSpec(
            num_scalar_prefetch=1,
            grid=(heads, tiles),
            in_specs=[
                tall,
                pl.BlockSpec((total, head_dim), lambda h, i, b: (0, h)),
                pl.BlockSpec((head_dim, total), lambda h, i, b: (h, 0)),
                pl.BlockSpec((total, head_dim), lambda h, i, b: (0, heads + h)),
                tall,
                row,
                row,
                stat,
                stat,
            ],
            out_specs=[pl.BlockSpec((head_dim, step), lambda h, i, b: (h, i)), pl.BlockSpec((2, total, head_dim), lambda h, i, b: (0, 0, h))],
            scratch_shapes=[pltpu.VMEM((total, step), jnp.float32), pltpu.VMEM((total, step), jnp.float32), pltpu.VMEM((1, step), jnp.float32)],
        ),
        out_shape=[
            jax.ShapeDtypeStruct((local_dim, span), jnp.float32),
            jax.ShapeDtypeStruct((2, total, local_dim), jnp.float32),
        ],
        compiler_params=pltpu.CompilerParams(vmem_limit_bytes=48 * 2**20),
        cost_estimate=pl.CostEstimate(flops=14 * span * total * local_dim, bytes_accessed=16 * total * local_dim, transcendentals=span * total * heads),
        name="attend_back",
    )(bounds, query, key_value, key_t, key_value, d_out, low, high, top, norm)


def solution(mesh):
    cp_count = mesh.shape["cp"]
    tp_count = mesh.shape["tp"]
    core_swap = [(i, i ^ 1) for i in range(cp_count)]
    chip_swap = [(i, i ^ (cp_count // 2)) for i in range(cp_count)]

    def device_step(tokens, pos, doc_id, dy, table, w_q, w_k, w_v, w_o, w_gate, w_up, w_down, gain_one, gain_two, inv_freq):
        span = tokens.shape[0]
        part = span // tp_count
        rows = table.shape[0]
        width = table.shape[1]
        head_dim = 2 * inv_freq.shape[0]
        heads = w_q.shape[1] // head_dim
        local_dim = heads * head_dim
        scale = head_dim ** -0.5
        tp_rank = lax.axis_index("tp")
        cp_rank = lax.axis_index("cp")
        core = cp_rank % 2
        gain_a = gain_one.astype(jnp.float32)
        gain_b = gain_two.astype(jnp.float32)

        def cp_sum(partial):
            half = partial.shape[0] // 2
            mine = lax.dynamic_slice_in_dim(partial, core * half, half, 0)
            other = lax.dynamic_slice_in_dim(partial, (1 - core) * half, half, 0)
            mate_part = lax.ppermute(other, "cp", core_swap)
            chip_half = mine + mate_part
            far_part = lax.ppermute(chip_half, "cp", chip_swap)
            total_half = chip_half + far_part
            other_half = lax.ppermute(total_half, "cp", core_swap)
            low = jnp.where(core == 0, total_half, other_half)
            high = jnp.where(core == 0, other_half, total_half)
            return jnp.concatenate([low, high], axis=0)

        ring_order = (tp_rank - jnp.arange(tp_count)) % tp_count
        half_dim = local_dim // 2
        wo_half = lax.dynamic_slice_in_dim(w_o, core * half_dim, half_dim, 0)
        wo_parts = [wo_half]
        for shift in range(1, tp_count):
            wo_parts.append(lax.ppermute(wo_half, "tp", [(i, (i + shift) % tp_count) for i in range(tp_count)]))
        wo_mine = jnp.concatenate(wo_parts, axis=0)
        wo_other = lax.ppermute(wo_mine, "cp", core_swap)
        wo_ring = jnp.concatenate([wo_mine, wo_other], axis=0)

        def to_ring(blocks):
            picked_blocks = jnp.take(blocks, ring_order, axis=0).reshape(tp_count, part, 2, half_dim)
            both = jnp.where(core == 0, picked_blocks, picked_blocks[:, :, ::-1])
            return both.transpose(1, 2, 0, 3).reshape(part, tp_count * local_dim)

        def from_ring(flat):
            both = flat.reshape(part, 2, tp_count, half_dim).transpose(2, 0, 1, 3)
            both = jnp.where(core == 0, both, both[:, :, ::-1]).reshape(tp_count, part, local_dim)
            return jnp.take(both, ring_order, axis=0)

        local_ids = tokens - tp_rank * rows
        owned = (local_ids >= 0) & (local_ids < rows)
        safe_ids = jnp.where(owned, local_ids, 0)
        picked = jnp.where(owned[:, None], jnp.take(table, safe_ids, axis=0), jnp.zeros((), jnp.bfloat16))
        embed = lax.psum_scatter(picked, "tp", scatter_dimension=0, tiled=True).astype(jnp.float32)

        normed_a, inv_a = rms_stats(embed)
        act_a = lax.all_gather((normed_a * gain_a).astype(jnp.bfloat16), "tp", axis=0, tiled=True)
        angle = pos.astype(jnp.float32)[:, None, None] * inv_freq
        cosine = jnp.cos(angle)
        sine = jnp.sin(angle)
        query = jnp.dot(act_a, w_q, preferred_element_type=jnp.float32).reshape(span, heads, head_dim)
        query = rotate(query, cosine, sine).astype(jnp.bfloat16).reshape(span, local_dim)
        key_loc = jnp.dot(act_a, w_k, preferred_element_type=jnp.float32).reshape(span, heads, head_dim)
        key_loc = rotate(key_loc, cosine, sine).astype(jnp.bfloat16)
        value_loc = jnp.dot(act_a, w_v, preferred_element_type=jnp.float32).astype(jnp.bfloat16)
        key_value = jnp.concatenate([key_loc.reshape(span, local_dim), value_loc], axis=1)
        kv_all = lax.all_gather(key_value, "cp", axis=0, tiled=True)
        kv_all_t = kv_all.T
        token_all = lax.all_gather(tokens, "cp", axis=0, tiled=True)
        q_seq = slot_sequence(cp_rank * span + jnp.arange(span, dtype=jnp.int32), span // 2, cp_count)
        q_first = q_seq - pos
        bounds = jnp.stack([jnp.min(q_first.reshape(-1, QUERY_STEP), axis=1), jnp.max(q_seq.reshape(-1, QUERY_STEP), axis=1)])
        low = q_first.reshape(1, span)
        high = q_seq.reshape(1, span)
        out_t, top, norm = attend(cp_count, scale, bounds, query, kv_all, kv_all_t, low, high)
        attended = out_t.T.astype(jnp.bfloat16)
        att_rows = lax.all_to_all(attended.reshape(tp_count, part, local_dim), "tp", 0, 0)
        residual = embed + jnp.dot(to_ring(att_rows), wo_ring, preferred_element_type=jnp.float32)
        normed_b, inv_b = rms_stats(residual)
        act_b = lax.all_gather((normed_b * gain_b).astype(jnp.bfloat16), "tp", axis=0, tiled=True)
        gate = jnp.dot(act_b, w_gate, preferred_element_type=jnp.float32)
        up_val = jnp.dot(act_b, w_up, preferred_element_type=jnp.float32)
        gate_sig = jax.nn.sigmoid(gate)
        hidden = (gate * gate_sig * up_val).astype(jnp.bfloat16)

        d_hidden = to_bf16(jnp.einsum("td,fd->tf", dy, w_down, preferred_element_type=jnp.float32))
        d_gate = (d_hidden * up_val * gate_sig * (1.0 + gate * (1.0 - gate_sig))).astype(jnp.bfloat16)
        d_up = (d_hidden * gate * gate_sig).astype(jnp.bfloat16)
        d_act_b = jnp.einsum("tf,df->td", d_gate, w_gate, preferred_element_type=jnp.float32)
        d_act_b = d_act_b + jnp.einsum("tf,df->td", d_up, w_up, preferred_element_type=jnp.float32)
        d_act_b = lax.psum_scatter(d_act_b, "tp", scatter_dimension=0, tiled=True)
        d_act_b = to_bf16(d_act_b)
        grad_gain_b = jnp.sum(d_act_b * normed_b, axis=0)
        dy_part = lax.dynamic_slice_in_dim(dy, tp_rank * part, part, 0).astype(jnp.float32)
        d_resid = dy_part + rms_back(d_act_b * gain_b, normed_b, inv_b)
        d_resid_b = d_resid.astype(jnp.bfloat16)
        d_att_rows = jnp.einsum("td,cd->tc", d_resid_b, wo_ring, preferred_element_type=jnp.float32)
        d_att = lax.all_to_all(from_ring(d_att_rows.astype(jnp.bfloat16)), "tp", 0, 0)
        d_att = d_att.reshape(span, local_dim)

        hidden_late = hidden
        grad_down = cp_sum(jnp.einsum("tf,td->fd", hidden, dy, preferred_element_type=jnp.float32))
        grad_gate = cp_sum(jnp.einsum("td,tf->df", act_b, d_gate, preferred_element_type=jnp.float32))
        grad_up = cp_sum(jnp.einsum("td,tf->df", act_b, d_up, preferred_element_type=jnp.float32))
        layer_part = jnp.dot(hidden_late, w_down, preferred_element_type=jnp.float32)
        layer_sum = lax.psum_scatter(layer_part, "tp", scatter_dimension=0, tiled=True)
        resid_all = lax.all_gather(d_resid_b, "tp", axis=0, tiled=True)
        grad_out = cp_sum(jnp.einsum("tc,td->cd", attended, resid_all, preferred_element_type=jnp.float32))

        d_query_t, d_kv_all = attend_back(cp_count, scale, bounds, query, kv_all, kv_all_t, d_att, low, high, top, norm)
        d_query = d_query_t.T.reshape(span, heads, head_dim)
        d_kv_all = d_kv_all.reshape(2, cp_count // 2, 2, span, local_dim)
        chip = cp_rank // 2
        mate_kv = lax.dynamic_index_in_dim(d_kv_all, 1 - core, 2, keepdims=False)
        own_kv = lax.dynamic_index_in_dim(d_kv_all, core, 2, keepdims=False)
        chip_kv = own_kv + lax.ppermute(mate_kv, "cp", core_swap)
        far_kv = lax.dynamic_index_in_dim(chip_kv, 1 - chip, 1, keepdims=False)
        d_kv = lax.dynamic_index_in_dim(chip_kv, chip, 1, keepdims=False) + lax.ppermute(far_kv, "cp", chip_swap)
        d_key = d_kv[0].reshape(span, heads, head_dim)
        d_value = d_kv[1]
        d_q_pre = rotate(to_bf16(d_query), cosine, -sine)
        d_q_pre = d_q_pre.astype(jnp.bfloat16).reshape(span, local_dim)
        d_k_pre = rotate(to_bf16(d_key), cosine, -sine).astype(jnp.bfloat16).reshape(span, local_dim)
        d_v_pre = d_value.astype(jnp.bfloat16).reshape(span, local_dim)
        grad_q = cp_sum(jnp.einsum("td,tc->dc", act_a, d_q_pre, preferred_element_type=jnp.float32))
        grad_k = cp_sum(jnp.einsum("td,tc->dc", act_a, d_k_pre, preferred_element_type=jnp.float32))
        grad_v = cp_sum(jnp.einsum("td,tc->dc", act_a, d_v_pre, preferred_element_type=jnp.float32))
        d_act_a = jnp.einsum("tc,dc->td", d_q_pre, w_q, preferred_element_type=jnp.float32)
        d_act_a = d_act_a + jnp.einsum("tc,dc->td", d_k_pre, w_k, preferred_element_type=jnp.float32)
        d_act_a = d_act_a + jnp.einsum("tc,dc->td", d_v_pre, w_v, preferred_element_type=jnp.float32)
        d_act_a, layer_sum = lax.optimization_barrier((d_act_a, layer_sum))
        d_act_a = lax.psum_scatter(d_act_a, "tp", scatter_dimension=0, tiled=True)
        d_act_a = to_bf16(d_act_a)
        layer_part = residual + layer_sum
        layer_out = lax.all_gather(layer_part.astype(jnp.bfloat16), "tp", axis=0, tiled=True)
        grad_gain_a = jnp.sum(d_act_a * normed_a, axis=0)
        d_embed = d_resid + rms_back(d_act_a * gain_a, normed_a, inv_a)
        embed_all = lax.all_gather(d_embed, ("cp", "tp"), axis=0, tiled=True)
        all_ids = token_all - tp_rank * rows
        drop_ids = jnp.where((all_ids >= 0) & (all_ids < rows), all_ids, rows)
        grad_table = jnp.zeros((rows, width), jnp.float32).at[drop_ids].add(embed_all, mode="drop")
        gains = lax.psum(jnp.stack([grad_gain_a, grad_gain_b]), ("tp", "cp"))
        return (layer_out, grad_table, grad_q, grad_k, grad_v, grad_out, grad_gate, grad_up, grad_down, gains[0], gains[1])

    col_spec = P(None, "tp")
    row_spec = P("tp", None)
    tok_spec = P("cp")
    rep_spec = P(None)
    in_specs = (tok_spec, tok_spec, tok_spec, P("cp", None), row_spec, col_spec, col_spec, col_spec, row_spec, col_spec, col_spec, row_spec, rep_spec, rep_spec, rep_spec)
    out_specs = (P("cp", None), row_spec, col_spec, col_spec, col_spec, row_spec, col_spec, col_spec, row_spec, rep_spec, rep_spec)

    return jax.shard_map(device_step, mesh=mesh, in_specs=in_specs, out_specs=out_specs, check_vma=False)
```

```python
import functools

import jax
import jax.numpy as jnp
from jax import lax
from jax.experimental import pallas as pl
from jax.experimental.pallas import tpu as pltpu
from jax.sharding import PartitionSpec as P


NORM_EPS = 1e-5
NEG_BIG = -1e30


def rms_stats(feats):
    inv_rms = lax.rsqrt(jnp.mean(feats * feats, axis=-1, keepdims=True) + NORM_EPS)
    return feats * inv_rms, inv_rms


def rms_back(d_normed, normed, inv_rms):
    return inv_rms * (d_normed - normed * jnp.mean(d_normed * normed, axis=-1, keepdims=True))


def rotate(tensor_in, cosine, sine):
    half = tensor_in.shape[-1] // 2
    first = tensor_in[..., :half]
    second = tensor_in[..., half:]
    return jnp.concatenate([first * cosine - second * sine, second * cosine + first * sine], axis=-1)


def to_bf16(feats):
    return feats.astype(jnp.bfloat16).astype(jnp.float32)


def slot_sequence(slot, block_len, cp_count):
    shard = slot // (2 * block_len)
    within = slot % (2 * block_len)
    block_no = jnp.where(within < block_len, shard, 2 * cp_count - 1 - shard)
    return block_no * block_len + within % block_len


KEY_STEP = 512
QUERY_STEP = 256
NT = (((1,), (1,)), ((), ()))
NN = (((1,), (0,)), ((), ()))


def block_number(index, cp_count):
    shard = index // 2
    return jnp.where(index % 2 == 0, shard, 2 * cp_count - 1 - shard)


def block_scores(key_ref, query, low, high, index, cp_count, scale):
    first = block_number(index, cp_count) * KEY_STEP
    keys = key_ref[pl.ds(pl.multiple_of(index * KEY_STEP, KEY_STEP), KEY_STEP), :]
    scores = lax.dot_general(keys, query, NT, preferred_element_type=jnp.float32) * scale
    seq = first + lax.broadcasted_iota(jnp.int32, scores.shape, 0)
    return jnp.where((seq >= low) & (seq <= high), scores, NEG_BIG)


def block_needed(index, tile_low, tile_high, cp_count):
    first = block_number(index, cp_count) * KEY_STEP
    return (first <= tile_high) & (first + KEY_STEP > tile_low)


def attend_kernel(cp_count, scale, bounds, query_ref, key_ref, value_t_ref, low_ref, high_ref, out_ref, top_ref, norm_ref, scores_ref):
    tile = pl.program_id(1)
    tile_low = bounds[0, tile]
    tile_high = bounds[1, tile]
    query = query_ref[...]
    low = low_ref[...]
    high = high_ref[...]
    count = key_ref.shape[0] // KEY_STEP
    step = query.shape[0]
    top_ref[0] = jnp.full((1, step), NEG_BIG, jnp.float32)

    def rows_of(index):
        return pl.ds(pl.multiple_of(index * KEY_STEP, KEY_STEP), KEY_STEP)

    @pl.loop(0, count)
    def _(index):
        @pl.when(block_needed(index, tile_low, tile_high, cp_count))
        def _():
            scores = block_scores(key_ref, query, low, high, index, cp_count, scale)
            scores_ref[rows_of(index), :] = scores
            top_ref[0] = jnp.maximum(top_ref[0], jnp.max(scores, axis=0, keepdims=True))

    norm_ref[0] = jnp.zeros((1, step), jnp.float32)

    @pl.loop(0, count)
    def _(index):
        @pl.when(block_needed(index, tile_low, tile_high, cp_count))
        def _():
            weight = jnp.exp(scores_ref[rows_of(index), :] - top_ref[0])
            scores_ref[rows_of(index), :] = weight
            norm_ref[0] = norm_ref[0] + jnp.sum(weight, axis=0, keepdims=True)

    norm_ref[0] = 1.0 / norm_ref[0]
    out_ref[...] = jnp.zeros_like(out_ref)

    @pl.loop(0, count)
    def _(index):
        @pl.when(block_needed(index, tile_low, tile_high, cp_count))
        def _():
            prob = (scores_ref[rows_of(index), :] * norm_ref[0]).astype(jnp.bfloat16)
            out_ref[...] += lax.dot_general(value_t_ref[:, rows_of(index)], prob, NN, preferred_element_type=jnp.float32)


def attend_back_kernel(cp_count, scale, bounds, query_ref, key_ref, key_t_ref, value_ref, d_out_ref, low_ref, high_ref, top_ref, norm_ref, d_query_ref, d_kv_ref, prob_ref, d_prob_ref, dot_ref):
    tile = pl.program_id(1)
    tile_low = bounds[0, tile]
    tile_high = bounds[1, tile]
    query = query_ref[...]
    d_out = d_out_ref[...]
    low = low_ref[...]
    high = high_ref[...]
    count = key_ref.shape[0] // KEY_STEP
    step = query.shape[0]

    def rows_of(index):
        return pl.ds(pl.multiple_of(index * KEY_STEP, KEY_STEP), KEY_STEP)

    @pl.when(tile == 0)
    def _():
        d_kv_ref[...] = jnp.zeros_like(d_kv_ref)

    dot_ref[...] = jnp.zeros((1, step), jnp.float32)

    @pl.loop(0, count)
    def _(index):
        @pl.when(block_needed(index, tile_low, tile_high, cp_count))
        def _():
            scores = block_scores(key_ref, query, low, high, index, cp_count, scale)
            prob = jnp.exp(scores - top_ref[0]) * norm_ref[0]
            d_prob = lax.dot_general(value_ref[rows_of(index), :], d_out, NT, preferred_element_type=jnp.float32)
            d_prob = d_prob.astype(jnp.bfloat16).astype(jnp.float32)
            prob_ref[rows_of(index), :] = prob
            d_prob_ref[rows_of(index), :] = d_prob
            dot_ref[...] += jnp.sum(prob * d_prob, axis=0, keepdims=True)

    d_query_ref[...] = jnp.zeros_like(d_query_ref)

    @pl.loop(0, count)
    def _(index):
        @pl.when(block_needed(index, tile_low, tile_high, cp_count))
        def _():
            prob = prob_ref[rows_of(index), :]
            d_scores = prob * (d_prob_ref[rows_of(index), :] - dot_ref[...]) * scale
            d_scores = d_scores.astype(jnp.bfloat16)
            d_query_ref[...] += lax.dot_general(key_t_ref[:, rows_of(index)], d_scores, NN, preferred_element_type=jnp.float32)
            d_kv_ref[0, rows_of(index), :] += lax.dot_general(d_scores, query, NN, preferred_element_type=jnp.float32)
            d_kv_ref[1, rows_of(index), :] += lax.dot_general(prob.astype(jnp.bfloat16), d_out, NN, preferred_element_type=jnp.float32)


def attend(cp_count, scale, bounds, query, key_value, value_t, low, high):
    span, local_dim = query.shape
    total = key_value.shape[0]
    head_dim = 128
    heads = local_dim // head_dim
    step = QUERY_STEP
    tiles = span // step
    row = pl.BlockSpec((1, step), lambda h, i, b: (0, i))
    stat = pl.BlockSpec((1, 1, step), lambda h, i, b: (h, 0, i))
    out_t, top, norm = pl.pallas_call(
        functools.partial(attend_kernel, cp_count, scale),
        grid_spec=pltpu.PrefetchScalarGridSpec(
            num_scalar_prefetch=1,
            grid=(heads, tiles),
            in_specs=[
                pl.BlockSpec((step, head_dim), lambda h, i, b: (i, h)),
                pl.BlockSpec((total, head_dim), lambda h, i, b: (0, h)),
                pl.BlockSpec((head_dim, total), lambda h, i, b: (heads + h, 0)),
                row,
                row,
            ],
            out_specs=[pl.BlockSpec((head_dim, step), lambda h, i, b: (h, i)), stat, stat],
            scratch_shapes=[pltpu.VMEM((total, step), jnp.float32)],
        ),
        out_shape=[
            jax.ShapeDtypeStruct((local_dim, span), jnp.float32),
            jax.ShapeDtypeStruct((heads, 1, span), jnp.float32),
            jax.ShapeDtypeStruct((heads, 1, span), jnp.float32),
        ],
        compiler_params=pltpu.CompilerParams(vmem_limit_bytes=40 * 2**20),
        cost_estimate=pl.CostEstimate(flops=6 * span * total * local_dim, bytes_accessed=8 * total * local_dim, transcendentals=span * total * heads),
        name="attend",
    )(bounds, query, key_value, value_t, low, high)
    return out_t, top, norm


def attend_back(cp_count, scale, bounds, query, key_value, key_t, d_out, low, high, top, norm):
    span, local_dim = query.shape
    total = key_value.shape[0]
    head_dim = 128
    heads = local_dim // head_dim
    step = QUERY_STEP
    tiles = span // step
    row = pl.BlockSpec((1, step), lambda h, i, b: (0, i))
    stat = pl.BlockSpec((1, 1, step), lambda h, i, b: (h, 0, i))
    tall = pl.BlockSpec((step, head_dim), lambda h, i, b: (i, h))
    return pl.pallas_call(
        functools.partial(attend_back_kernel, cp_count, scale),
        grid_spec=pltpu.PrefetchScalarGridSpec(
            num_scalar_prefetch=1,
            grid=(heads, tiles),
            in_specs=[
                tall,
                pl.BlockSpec((total, head_dim), lambda h, i, b: (0, h)),
                pl.BlockSpec((head_dim, total), lambda h, i, b: (h, 0)),
                pl.BlockSpec((total, head_dim), lambda h, i, b: (0, heads + h)),
                tall,
                row,
                row,
                stat,
                stat,
            ],
            out_specs=[pl.BlockSpec((head_dim, step), lambda h, i, b: (h, i)), pl.BlockSpec((2, total, head_dim), lambda h, i, b: (0, 0, h))],
            scratch_shapes=[pltpu.VMEM((total, step), jnp.float32), pltpu.VMEM((total, step), jnp.float32), pltpu.VMEM((1, step), jnp.float32)],
        ),
        out_shape=[
            jax.ShapeDtypeStruct((local_dim, span), jnp.float32),
            jax.ShapeDtypeStruct((2, total, local_dim), jnp.float32),
        ],
        compiler_params=pltpu.CompilerParams(vmem_limit_bytes=48 * 2**20),
        cost_estimate=pl.CostEstimate(flops=14 * span * total * local_dim, bytes_accessed=16 * total * local_dim, transcendentals=span * total * heads),
        name="attend_back",
    )(bounds, query, key_value, key_t, key_value, d_out, low, high, top, norm)


def solution(mesh):
    cp_count = mesh.shape["cp"]
    tp_count = mesh.shape["tp"]
    core_swap = [(i, i ^ 1) for i in range(cp_count)]
    chip_swap = [(i, i ^ (cp_count // 2)) for i in range(cp_count)]

    def device_step(tokens, pos, doc_id, dy, table, w_q, w_k, w_v, w_o, w_gate, w_up, w_down, gain_one, gain_two, inv_freq):
        span = tokens.shape[0]
        part = span // tp_count
        rows = table.shape[0]
        width = table.shape[1]
        head_dim = 2 * inv_freq.shape[0]
        heads = w_q.shape[1] // head_dim
        local_dim = heads * head_dim
        scale = head_dim ** -0.5
        tp_rank = lax.axis_index("tp")
        cp_rank = lax.axis_index("cp")
        core = cp_rank % 2
        gain_a = gain_one.astype(jnp.float32)
        gain_b = gain_two.astype(jnp.float32)

        def cp_sum(partial):
            half = partial.shape[0] // 2
            mine = lax.dynamic_slice_in_dim(partial, core * half, half, 0)
            other = lax.dynamic_slice_in_dim(partial, (1 - core) * half, half, 0)
            mate_part = lax.ppermute(other, "cp", core_swap)
            chip_half = mine + mate_part
            far_part = lax.ppermute(chip_half, "cp", chip_swap)
            total_half = chip_half + far_part
            other_half = lax.ppermute(total_half, "cp", core_swap)
            low = jnp.where(core == 0, total_half, other_half)
            high = jnp.where(core == 0, other_half, total_half)
            return jnp.concatenate([low, high], axis=0)

        ring_order = (tp_rank - jnp.arange(tp_count)) % tp_count
        half_dim = local_dim // 2
        wo_half = lax.dynamic_slice_in_dim(w_o, core * half_dim, half_dim, 0)
        wo_parts = [wo_half]
        for shift in range(1, tp_count):
            wo_parts.append(lax.ppermute(wo_half, "tp", [(i, (i + shift) % tp_count) for i in range(tp_count)]))
        wo_mine = jnp.concatenate(wo_parts, axis=0)
        wo_other = lax.ppermute(wo_mine, "cp", core_swap)
        wo_ring = jnp.concatenate([wo_mine, wo_other], axis=0)

        def to_ring(blocks):
            picked_blocks = jnp.take(blocks, ring_order, axis=0).reshape(tp_count, part, 2, half_dim)
            both = jnp.where(core == 0, picked_blocks, picked_blocks[:, :, ::-1])
            return both.transpose(1, 2, 0, 3).reshape(part, tp_count * local_dim)

        def from_ring(flat):
            both = flat.reshape(part, 2, tp_count, half_dim).transpose(2, 0, 1, 3)
            both = jnp.where(core == 0, both, both[:, :, ::-1]).reshape(tp_count, part, local_dim)
            return jnp.take(both, ring_order, axis=0)

        local_ids = tokens - tp_rank * rows
        owned = (local_ids >= 0) & (local_ids < rows)
        safe_ids = jnp.where(owned, local_ids, 0)
        picked = jnp.where(owned[:, None], jnp.take(table, safe_ids, axis=0), jnp.zeros((), jnp.bfloat16))
        embed = lax.psum_scatter(picked, "tp", scatter_dimension=0, tiled=True).astype(jnp.float32)

        normed_a, inv_a = rms_stats(embed)
        act_a = lax.all_gather((normed_a * gain_a).astype(jnp.bfloat16), "tp", axis=0, tiled=True)
        angle = pos.astype(jnp.float32)[:, None, None] * inv_freq
        cosine = jnp.cos(angle)
        sine = jnp.sin(angle)
        cos_row = jnp.tile(cosine[:, 0], (1, 2 * heads))
        sin_row = jnp.tile(sine[:, 0], (1, 2 * heads))

        def project(weight):
            pairs = weight.reshape(width, heads, 2, head_dim // 2)
            turned = jnp.stack([-pairs[:, :, 1], pairs[:, :, 0]], axis=2).reshape(width, local_dim)
            straight = jnp.dot(act_a, weight, preferred_element_type=jnp.float32)
            crossed = jnp.dot(act_a, turned, preferred_element_type=jnp.float32)
            return (straight * cos_row + crossed * sin_row).astype(jnp.bfloat16)

        query = project(w_q)
        key_loc = project(w_k)
        value_loc = jnp.dot(act_a, w_v, preferred_element_type=jnp.float32).astype(jnp.bfloat16)
        key_value = jnp.concatenate([key_loc, value_loc], axis=1)
        kv_all = lax.all_gather(key_value, "cp", axis=0, tiled=True)
        kv_all_t = kv_all.T
        token_all = lax.all_gather(tokens, "cp", axis=0, tiled=True)
        q_seq = slot_sequence(cp_rank * span + jnp.arange(span, dtype=jnp.int32), span // 2, cp_count)
        q_first = q_seq - pos
        bounds = jnp.stack([jnp.min(q_first.reshape(-1, QUERY_STEP), axis=1), jnp.max(q_seq.reshape(-1, QUERY_STEP), axis=1)])
        low = q_first.reshape(1, span)
        high = q_seq.reshape(1, span)
        out_t, top, norm = attend(cp_count, scale, bounds, query, kv_all, kv_all_t, low, high)
        attended = out_t.T.astype(jnp.bfloat16)
        att_rows = lax.all_to_all(attended.reshape(tp_count, part, local_dim), "tp", 0, 0)
        residual = embed + jnp.dot(to_ring(att_rows), wo_ring, preferred_element_type=jnp.float32)
        normed_b, inv_b = rms_stats(residual)
        act_b = lax.all_gather((normed_b * gain_b).astype(jnp.bfloat16), "tp", axis=0, tiled=True)
        gate = jnp.dot(act_b, w_gate, preferred_element_type=jnp.float32)
        up_val = jnp.dot(act_b, w_up, preferred_element_type=jnp.float32)
        gate_sig = jax.nn.sigmoid(gate)
        hidden = (gate * gate_sig * up_val).astype(jnp.bfloat16)

        d_hidden = to_bf16(jnp.einsum("td,fd->tf", dy, w_down, preferred_element_type=jnp.float32))
        d_gate = (d_hidden * up_val * gate_sig * (1.0 + gate * (1.0 - gate_sig))).astype(jnp.bfloat16)
        d_up = (d_hidden * gate * gate_sig).astype(jnp.bfloat16)
        d_act_b = jnp.einsum("tf,df->td", d_gate, w_gate, preferred_element_type=jnp.float32)
        d_act_b = d_act_b + jnp.einsum("tf,df->td", d_up, w_up, preferred_element_type=jnp.float32)
        d_act_b = lax.psum_scatter(d_act_b, "tp", scatter_dimension=0, tiled=True)
        d_act_b = to_bf16(d_act_b)
        grad_gain_b = jnp.sum(d_act_b * normed_b, axis=0)
        dy_part = lax.dynamic_slice_in_dim(dy, tp_rank * part, part, 0).astype(jnp.float32)
        d_resid = dy_part + rms_back(d_act_b * gain_b, normed_b, inv_b)
        d_resid_b = d_resid.astype(jnp.bfloat16)
        d_att_rows = jnp.einsum("td,cd->tc", d_resid_b, wo_ring, preferred_element_type=jnp.float32)
        d_att = lax.all_to_all(from_ring(d_att_rows.astype(jnp.bfloat16)), "tp", 0, 0)
        d_att = d_att.reshape(span, local_dim)

        hidden_late = hidden
        grad_down = cp_sum(jnp.einsum("tf,td->fd", hidden, dy, preferred_element_type=jnp.float32))
        grad_gate = cp_sum(jnp.einsum("td,tf->df", act_b, d_gate, preferred_element_type=jnp.float32))
        grad_up = cp_sum(jnp.einsum("td,tf->df", act_b, d_up, preferred_element_type=jnp.float32))
        layer_part = jnp.dot(hidden_late, w_down, preferred_element_type=jnp.float32)
        layer_sum = lax.psum_scatter(layer_part, "tp", scatter_dimension=0, tiled=True)
        resid_all = lax.all_gather(d_resid_b, "tp", axis=0, tiled=True)
        grad_out = cp_sum(jnp.einsum("tc,td->cd", attended, resid_all, preferred_element_type=jnp.float32))

        d_query_t, d_kv_all = attend_back(cp_count, scale, bounds, query, kv_all, kv_all_t, d_att, low, high, top, norm)
        d_query = d_query_t.T.reshape(span, heads, head_dim)
        d_kv_all = d_kv_all.reshape(2, cp_count // 2, 2, span, local_dim)
        chip = cp_rank // 2
        mate_kv = lax.dynamic_index_in_dim(d_kv_all, 1 - core, 2, keepdims=False)
        own_kv = lax.dynamic_index_in_dim(d_kv_all, core, 2, keepdims=False)
        chip_kv = own_kv + lax.ppermute(mate_kv, "cp", core_swap)
        far_kv = lax.dynamic_index_in_dim(chip_kv, 1 - chip, 1, keepdims=False)
        d_kv = lax.dynamic_index_in_dim(chip_kv, chip, 1, keepdims=False) + lax.ppermute(far_kv, "cp", chip_swap)
        d_key = d_kv[0].reshape(span, heads, head_dim)
        d_value = d_kv[1]
        d_q_pre = rotate(to_bf16(d_query), cosine, -sine)
        d_q_pre = d_q_pre.astype(jnp.bfloat16).reshape(span, local_dim)
        d_k_pre = rotate(to_bf16(d_key), cosine, -sine).astype(jnp.bfloat16).reshape(span, local_dim)
        d_v_pre = d_value.astype(jnp.bfloat16).reshape(span, local_dim)
        grad_q = cp_sum(jnp.einsum("td,tc->dc", act_a, d_q_pre, preferred_element_type=jnp.float32))
        grad_k = cp_sum(jnp.einsum("td,tc->dc", act_a, d_k_pre, preferred_element_type=jnp.float32))
        grad_v = cp_sum(jnp.einsum("td,tc->dc", act_a, d_v_pre, preferred_element_type=jnp.float32))
        d_act_a = jnp.einsum("tc,dc->td", d_q_pre, w_q, preferred_element_type=jnp.float32)
        d_act_a = d_act_a + jnp.einsum("tc,dc->td", d_k_pre, w_k, preferred_element_type=jnp.float32)
        d_act_a = d_act_a + jnp.einsum("tc,dc->td", d_v_pre, w_v, preferred_element_type=jnp.float32)
        d_act_a, layer_sum = lax.optimization_barrier((d_act_a, layer_sum))
        d_act_a = lax.psum_scatter(d_act_a, "tp", scatter_dimension=0, tiled=True)
        d_act_a = to_bf16(d_act_a)
        layer_part = residual + layer_sum
        layer_out = lax.all_gather(layer_part.astype(jnp.bfloat16), "tp", axis=0, tiled=True)
        grad_gain_a = jnp.sum(d_act_a * normed_a, axis=0)
        d_embed = d_resid + rms_back(d_act_a * gain_a, normed_a, inv_a)
        embed_all = lax.all_gather(d_embed, ("cp", "tp"), axis=0, tiled=True)
        all_ids = token_all - tp_rank * rows
        drop_ids = jnp.where((all_ids >= 0) & (all_ids < rows), all_ids, rows)
        grad_table = jnp.zeros((rows, width), jnp.float32).at[drop_ids].add(embed_all, mode="drop")
        gains = lax.psum(jnp.stack([grad_gain_a, grad_gain_b]), ("tp", "cp"))
        return (layer_out, grad_table, grad_q, grad_k, grad_v, grad_out, grad_gate, grad_up, grad_down, gains[0], gains[1])

    col_spec = P(None, "tp")
    row_spec = P("tp", None)
    tok_spec = P("cp")
    rep_spec = P(None)
    in_specs = (tok_spec, tok_spec, tok_spec, P("cp", None), row_spec, col_spec, col_spec, col_spec, row_spec, col_spec, col_spec, row_spec, rep_spec, rep_spec, rep_spec)
    out_specs = (P("cp", None), row_spec, col_spec, col_spec, col_spec, row_spec, col_spec, col_spec, row_spec, rep_spec, rep_spec)

    return jax.shard_map(device_step, mesh=mesh, in_specs=in_specs, out_specs=out_specs, check_vma=False)
```
